32 devices in a mesh: shard: 2 (over core), cols: 4 (over y, x), job: 4 (over z).
Axes of the slice: x: 2, y: 2, z: 4, core: 2. Of those that a mesh axis runs over, the one named last changes fastest.
Arguments:
- one_query: float32 [16384, 4096], P(('job', 'shard'), 'cols'), parts along dimension 0, may hold values from -0.125 to 0.125
- other_query: float32 [16384, 4096], P(('job', 'shard'), 'cols'), parts along dimension 0, may hold values from -0.09375 to 0.09375
- one_key: float32 [16384, 1024], P(('job', 'shard'), 'cols'), parts along dimension 0, may hold values from -0.125 to 0.125
- other_key: float32 [16384, 1024], P(('job', 'shard'), 'cols'), parts along dimension 0, may hold values from -0.09375 to 0.09375
- one_value: float32 [16384, 1024], P(('job', 'shard'), 'cols'), parts along dimension 0, may hold values from -0.125 to 0.125
- other_value: float32 [16384, 1024], P(('job', 'shard'), 'cols'), parts along dimension 0, may hold values from -0.09375 to 0.09375
- mix_share: float32 [16384], P(('job', 'shard')), parts along dimension 0, may hold values from 0.2 to 0.8
- norm_gain: float32 [16384], P(('job', 'shard')), parts along dimension 0, may hold values from 0.25 to 1.75
Outputs:
- final_query: bfloat16 [16384, 4096], P('job', 'cols'), parts along dimension 0
- final_key: bfloat16 [16384, 1024], P('job', 'cols'), parts along dimension 0
- final_value: bfloat16 [16384, 1024], P('job', 'cols'), parts along dimension 0
- scale_query: float32 [16384], P(('job', 'cols')), parts along dimension 0
- scale_key: float32 [4096], P(('job', 'cols')), parts along dimension 0
- scale_value: float32 [4096], P(('job', 'cols')), parts along dimension 0
The draws below stay inside these ranges and needn't reach their ends.
There are 4 independent parts, one for each index of `job`. The reference program is written for one: setup_inputs(seed, part) draws one part's arguments, and reference() takes and returns one part's arrays. A program takes and returns all parts, laid end to end along the dimension named above; each array names one. Nothing has to cross between parts.
All inputs are finite; a program needn't handle non-finite values. Where the reference program divides by a largest or mean magnitude, that divisor is 1e-20 or more.
Results may differ from the reference program's by a relative error of at most 0.001.
Values may be sent and summed in bfloat16 or wider, within the bound.
No kernel may reach another device: no remote copies, remote signals or barrier semaphores. Data moves between devices by JAX's collectives and lax.ppermute only.
A program may use at most 128 MiB of HBM per device.

```python
import jax
import jax.numpy as jnp

D_MODEL = 4096
Q_DIM = 4096
KV_DIM = 1024


def strengthened(drawn, rng, source, target, blocks, factor):
    def block_of(position):
        return (jnp.arange(drawn.shape[position]) // (drawn.shape[position] // blocks)).reshape((-1,) + (1,) * (drawn.ndim - 1 - position))

    one_side = jax.random.permutation(rng, blocks)[block_of(target)]
    second = (block_of(target) + blocks // 2) % blocks
    return jnp.where((block_of(source) == one_side) | (block_of(source) == second), factor * drawn, drawn)


def level_of(own_key, shape, shards, smallest, high):
    def one(position, blocks):
        steps = jax.random.uniform(jax.random.fold_in(jax.random.fold_in(own_key, 6), position), (blocks,), jnp.float32, smallest / len(shards), high / len(shards))
        return jnp.repeat(jnp.exp(steps), shape[position] // blocks).reshape((-1,) + (1,) * (len(shape) - position - 1))

    factor_of = one(*shards[0])
    for cut in shards[1:]:
        factor_of = factor_of * one(*cut)
    return factor_of


def normal_values(key, shape, width, most, cuts=(), dtype=jnp.bfloat16):
    array = width * jax.random.normal(key, shape, jnp.float32)
    if cuts:
        array = array * level_of(key, shape, cuts, -0.22, 0.18)
    return jnp.clip(array, -most, most).astype(dtype)


def noise_with(stream_key, shape, scale, bound, pieces, heavy, dtype=jnp.bfloat16):
    entries = scale * jax.random.normal(stream_key, shape, jnp.float32)
    if pieces:
        entries = entries * level_of(stream_key, shape, pieces, -0.22, 0.18)
    return jnp.clip(strengthened(entries, jax.random.fold_in(stream_key, 3), *heavy), -bound, bound).astype(dtype)


def setup_inputs(seed: int = 0, part: int = 0) -> dict:
    arg_keys = jax.random.split(jax.random.key(seed), 9)
    part_keys = jax.random.split(jax.random.fold_in(arg_keys[8], part), 9)
    return {
        "one_query": noise_with(part_keys[0], (D_MODEL, Q_DIM), D_MODEL ** -0.5, 0.125, ((0, 2), (1, 4)), (0, 1, 4, 2.0), jnp.float32),
        "other_query": normal_values(part_keys[1], (D_MODEL, Q_DIM), D_MODEL ** -0.5, 0.09375, ((0, 2), (1, 4)), jnp.float32),
        "one_key": noise_with(part_keys[2], (D_MODEL, KV_DIM), D_MODEL ** -0.5, 0.125, ((0, 2), (1, 4)), (0, 1, 4, 2.0), jnp.float32),
        "other_key": normal_values(part_keys[3], (D_MODEL, KV_DIM), D_MODEL ** -0.5, 0.09375, ((0, 2), (1, 4)), jnp.float32),
        "one_value": noise_with(part_keys[4], (D_MODEL, KV_DIM), D_MODEL ** -0.5, 0.125, ((0, 2), (1, 4)), (0, 1, 4, 2.0), jnp.float32),
        "other_value": normal_values(part_keys[5], (D_MODEL, KV_DIM), D_MODEL ** -0.5, 0.09375, ((0, 2), (1, 4)), jnp.float32),
        "mix_share": jnp.clip(0.2 + 0.6 * jax.random.uniform(part_keys[6], (D_MODEL,), jnp.float32) ** level_of(part_keys[6], (D_MODEL,), ((0, 2),), -0.2, 0.2), 0.2, 0.8),
        "norm_gain": jnp.clip(1.0 + 0.15 * jax.random.normal(part_keys[7], (D_MODEL,), jnp.float32), 0.25, 1.75),
    }


def reference(one_query, other_query, one_key, other_key, one_value, other_value, mix_share, norm_gain):
    result_query = mix_share[:, None] * one_query + (1.0 - mix_share[:, None]) * other_query
    result_key = mix_share[:, None] * one_key + (1.0 - mix_share[:, None]) * other_key
    result_value = mix_share[:, None] * one_value + (1.0 - mix_share[:, None]) * other_value
    result_gained_query = result_query * norm_gain[:, None]
    result_gained_key = result_key * norm_gain[:, None]
    result_gained_value = result_value * norm_gain[:, None]
    scale_query = jnp.max(jnp.abs(result_gained_query), axis=0)
    final_query = (result_gained_query / scale_query).astype(jnp.bfloat16)
    scale_key = jnp.max(jnp.abs(result_gained_key), axis=0)
    final_key = (result_gained_key / scale_key).astype(jnp.bfloat16)
    scale_value = jnp.max(jnp.abs(result_gained_value), axis=0)
    final_value = (result_gained_value / scale_value).astype(jnp.bfloat16)
    return final_query, final_key, final_value, scale_query, scale_key, scale_value
```

```python
import jax
import jax.numpy as jnp
from jax import lax
from jax.experimental import pallas as pl
from jax.experimental.pallas import tpu as pltpu
from jax.sharding import PartitionSpec as P

AXIS = "shard"
COST0 = 6_000_000_000
COST = 1000
LANES = 128
BLOCK = 256
ROWS = 16
UNROLL = 8
CUTS = ((0, 1, 0), (0, 0, 1), (2, 0, 0), (3, 0, 0), (3, 0, 0))
PLAN = (dict(spread=1,mix=0), dict(mix=1), dict(slim=0), dict(slim=1), dict(mix=2), dict(mix=3, own=(0,)), dict(slim=2), dict(slim=3), dict(mix=4, own=(1,), got=(0,)), dict(own=(2,), got=(1,)), dict(slim=4), dict(own=(3,4), got=(2,), scales=1), dict(got=(3,)), dict(got=(4,)))
FETCHED = (1,)
RESIDENT = ()


def in_vmem(x):
    return pltpu.with_memory_space_constraint(x, pltpu.VMEM)


def in_hbm(x):
    return pltpu.with_memory_space_constraint(x, pltpu.HBM)


def parts_of(cuts, widths):
    total = [sum(c[a] for c in cuts) for a in range(len(widths))]
    done = [0] * len(widths)
    chunks = []
    for cut in cuts:
        parts = []
        for a, units in enumerate(cut):
            if units:
                cols = widths[a] * units // total[a]
                parts.append((a, done[a], cols))
                done[a] += cols
        chunks.append(tuple(parts))
    return chunks


def width_of(parts):
    return sum(cols for _, _, cols in parts)


class Call:
    def __init__(self):
        self.args, self.in_specs, self.names = [], [], []
        self.outs, self.out_specs, self.out_names = [], [], []
        self.scratch, self.scratch_names = [], []
        self.aliases = {}

    def take(self, name, x, space):
        if name in self.names:
            return
        if space is pltpu.VMEM:
            x = in_vmem(x)
        elif space is pltpu.HBM:
            x = in_hbm(x)
        self.args.append(x)
        self.in_specs.append(pl.BlockSpec(memory_space=space))
        self.names.append(name)

    def give(self, name, shape, space):
        self.outs.append(shape)
        self.out_specs.append(pl.BlockSpec(memory_space=space))
        self.out_names.append(name)

    def hold(self, name, shape):
        self.scratch.append(shape)
        self.scratch_names.append(name)

    def run(self, body, vmem, token_name=1):
        def kernel(*refs):
            body(dict(zip(self.names + self.out_names + self.scratch_names, refs)))

        out = pl.pallas_call(
            kernel,
            out_shape=tuple(self.outs),
            in_specs=self.in_specs,
            out_specs=tuple(self.out_specs),
            scratch_shapes=self.scratch,
            input_output_aliases=self.aliases,
            compiler_params=pltpu.CompilerParams(vmem_limit_bytes=vmem),
            cost_estimate=pl.CostEstimate(flops=COST0 if token_name == 0 else COST, bytes_accessed=0, transcendentals=0),
        )(*self.args)
        return dict(zip(self.out_names, out))


def column(row):
    return jnp.broadcast_to(row, (LANES, LANES)).T


def make(n):
    def shards(*arrays):
        return compute(n, arrays)

    return shards


def compute(n, arrays):
    pairs = [arrays[0:2], arrays[2:4], arrays[4:6]]
    share, gain = arrays[6:8]
    rows = share.shape[0]
    block = min(BLOCK, rows)
    blocks = rows // block
    widths = [p[0].shape[1] for p in pairs]
    chunks = parts_of(CUTS, widths)
    count = len(chunks)
    perms = [[(i, (i + k) % n) for i in range(n)] for k in range(1, n)]
    f32, b16 = jnp.float32, jnp.bfloat16
    VMEM, HBM = pltpu.VMEM, pltpu.HBM

    kept, peaks, narrow, pieces, finals = {}, {}, {}, {}, {}
    columns = token = scales = None
    for step, plan in enumerate(PLAN):
        spread = "spread" in plan
        mix = chunks[plan["mix"]] if "mix" in plan else None
        slim = plan.get("slim")
        own, put = plan.get("own", ()), plan.get("got", ())
        call = Call()
        held = 0
        if token is not None:
            call.take("token_in", token, VMEM)
        call.give("token", VMEM((8, LANES), f32), VMEM)
        if spread:
            call.take("share_row", share.reshape(rows // LANES, LANES), HBM)
            call.take("gain_row", gain.reshape(rows // LANES, LANES), HBM)
            call.give("share", VMEM((rows, LANES), f32), VMEM)
            call.give("gain", VMEM((rows, LANES), f32), VMEM)
            call.hold("share_lanes", VMEM((rows // LANES, LANES), f32))
            call.hold("gain_lanes", VMEM((rows // LANES, LANES), f32))
            call.hold("row_sem", pltpu.SemaphoreType.DMA((2,)))
        if mix:
            for p, (a, _, cols) in enumerate(mix):
                space = HBM if a in FETCHED else VMEM
                call.take(f"one{a}", pairs[a][0], space)
                call.take(f"other{a}", pairs[a][1], space)
                if a in FETCHED:
                    call.hold(f"in{p}", VMEM((2, rows, cols), f32))
                    held += 2 * rows * cols * 4
            if not spread:
                call.take("share", columns[0], VMEM)
                call.take("gain", columns[1], VMEM)
            w = width_of(mix)
            call.give("kept", VMEM((rows, w), f32), VMEM)
            call.give("peak", VMEM((1, w), f32), VMEM)
            fetch = [p for p, (a, _, _) in enumerate(mix) if a in FETCHED]
            if fetch:
                call.hold("in_sem", pltpu.SemaphoreType.DMA((len(mix), 2, blocks)))
        if slim is not None:
            call.take("full", kept[slim], VMEM)
            for k, x in enumerate(peaks[slim]):
                call.take(f"top{k}", x, VMEM)
            call.give("narrow", VMEM(kept[slim].shape, b16), VMEM)
        if "scales" in plan:
            for c in range(count):
                for k, x in enumerate(peaks[c]):
                    call.take(f"top{c}_{k}", x, VMEM)
            for a, wd in enumerate(widths):
                call.give(f"scale{a}", jax.ShapeDtypeStruct((1, wd), f32), pl.ANY)
                call.hold(f"scale_rows{a}", VMEM((1, wd), f32))
            call.hold("scale_sem", pltpu.SemaphoreType.DMA((len(widths),)))
        for c in own:
            if c != slim:
                call.take(f"own{c}", narrow[c], VMEM)
        for c in put:
            for k, x in enumerate(pieces[c]):
                call.take(f"piece{c}_{k}", x, VMEM)
        moves = [(c, 0) for c in own] + [(c, k) for c in put for k in range(1, n)]
        moves = [(c, k, p) for c, k in moves for p in range(len(chunks[c]))]
        inner = [m for m in moves if chunks[m[0]][m[2]][0] in RESIDENT]
        moves = [m for m in moves if m not in inner]
        if moves:
            call.hold("out_sem", pltpu.SemaphoreType.DMA((len(moves),)))
        touched = sorted({chunks[c][p][0] for c, _, p in moves + inner})
        for a in touched:
            whole, space = jax.ShapeDtypeStruct((rows * n, widths[a]), b16), pl.ANY
            if a in RESIDENT:
                whole, space = VMEM((rows * n, widths[a]), b16), VMEM
            if a in finals:
                call.aliases[len(call.args)] = len(call.outs)
                call.take(f"was{a}", finals[a], space)
            call.give(f"final{a}", whole, space)

        def body(r, mix=mix, slim=slim, put=put, step=step, spread=spread, moves=moves, plan=plan, inner=inner):
            reads, writes = {}, []
            if spread:
                vecs = [
                    pltpu.make_async_copy(r[f"{nm}_row"], r[f"{nm}_lanes"], r["row_sem"].at[i])
                    for i, nm in enumerate(("share", "gain"))
                ]
                for c in vecs:
                    c.start()
            if mix:
                for b in range(blocks):
                    at = pl.ds(b * block, block)
                    for p, (a, start, cols) in enumerate(mix):
                        if a in FETCHED:
                            for k, nm in enumerate(("one", "other")):
                                c = pltpu.make_async_copy(
                                    r[f"{nm}{a}"].at[at, pl.ds(start, cols)],
                                    r[f"in{p}"].at[k, at, :],
                                    r["in_sem"].at[p, k, b],
                                )
                                c.start()
                                reads[p, k, b] = c
            me = lax.axis_index(AXIS)

            def rows_of(k):
                return pl.ds(pl.multiple_of(lax.rem(me + n - k, n) * rows, rows), rows)

            def move(i):
                c, k, p = moves[i]
                base = sum(cols for _, _, cols in chunks[c][:p])
                a, start, cols = chunks[c][p]
                src = r[f"piece{c}_{k - 1}"] if k else r["narrow"] if c == slim else r[f"own{c}"]
                x = pltpu.make_async_copy(
                    src.at[:, pl.ds(base, cols)],
                    r[f"final{a}"].at[rows_of(k), pl.ds(start, cols)],
                    r["out_sem"].at[i],
                )
                x.start()
                writes.append(x)

            for i, (c, k, _) in enumerate(moves):
                if k or c != slim:
                    move(i)
            if slim is not None:
                top = r["top0"][...]
                for k in range(1, n):
                    top = jnp.maximum(top, r[f"top{k}"][...])
                inv = 1.0 / top

                def slim_rows(i, _):
                    at = pl.ds(pl.multiple_of(i * 64, 64), 64)
                    r["narrow"][at, :] = (r["full"][at, :] * inv).astype(b16)
                    return 0

                lax.fori_loop(0, rows // 64, slim_rows, 0)
                for i, (c, k, _) in enumerate(moves):
                    if not k and c == slim:
                        move(i)
            for c, k, p in inner:
                base = sum(cols for _, _, cols in chunks[c][:p])
                a, start, cols = chunks[c][p]
                src = r[f"piece{c}_{k - 1}"] if k else r["narrow"] if c == slim else r[f"own{c}"]
                first = lax.rem(me + n - k, n) * rows

                def copy_rows(i, _, src=src, a=a, start=start, cols=cols, base=base, first=first):
                    at = pl.ds(pl.multiple_of(i * 128, 128), 128)
                    to = pl.ds(pl.multiple_of(first + i * 128, 128), 128)
                    r[f"final{a}"][to, start : start + cols] = src[at, base : base + cols]
                    return 0

                lax.fori_loop(0, rows // 128, copy_rows, 0)
            if "scales" in plan:
                for c in range(count):
                    t = r[f"top{c}_0"][...]
                    for k in range(1, n):
                        t = jnp.maximum(t, r[f"top{c}_{k}"][...])
                    base = 0
                    for a, start, cols in chunks[c]:
                        r[f"scale_rows{a}"][:, start : start + cols] = t[:, base : base + cols]
                        base += cols
                for a in range(len(widths)):
                    x = pltpu.make_async_copy(r[f"scale_rows{a}"], r[f"scale{a}"], r["scale_sem"].at[a])
                    x.start()
                    writes.append(x)
            if spread:
                for c in vecs:
                    c.wait()
                for t in range(rows // LANES):
                    at = slice(t * LANES, (t + 1) * LANES)
                    m = r["share_lanes"][t : t + 1, :]
                    g = r["gain_lanes"][t : t + 1, :]
                    r["share"][at, :] = column(m * g)
                    r["gain"][at, :] = column((1.0 - m) * g)
            if mix:
                w = width_of(mix)
                acc = tuple(jnp.zeros((8, LANES), f32) for _ in range(w // LANES))
                fetched = any(a in FETCHED for a, _, _ in mix)
                chunk = block if fetched else rows
                for b in range(rows // chunk):
                    for p, (a, _, _) in enumerate(mix):
                        if a in FETCHED:
                            for k in range(2):
                                reads[p, k, b].wait()

                    def mix_rows(i, acc, b=b):
                        at = pl.ds(pl.multiple_of(b * chunk + i * ROWS, ROWS), ROWS)
                        s = r["share"][at, :]
                        o = r["gain"][at, :]
                        acc = list(acc)
                        j = 0
                        for p, (a, start, cols) in enumerate(mix):
                            for c in range(0, cols, LANES):
                                if a in FETCHED:
                                    x = r[f"in{p}"][0, at, c : c + LANES]
                                    y = r[f"in{p}"][1, at, c : c + LANES]
                                else:
                                    x = r[f"one{a}"][at, start + c : start + c + LANES]
                                    y = r[f"other{a}"][at, start + c : start + c + LANES]
                                v = s * x + o * y
                                r["kept"][at, j * LANES : (j + 1) * LANES] = v
                                m = jnp.abs(v)
                                for q in range(0, ROWS, 8):
                                    acc[j] = jnp.maximum(acc[j], m[q : q + 8])
                                j += 1
                        return tuple(acc)

                    acc = lax.fori_loop(0, chunk // ROWS, mix_rows, acc, unroll=min(UNROLL, chunk // ROWS))
                for j, m in enumerate(acc):
                    r["peak"][:, j * LANES : (j + 1) * LANES] = jnp.max(m, axis=0, keepdims=True)
            for c in writes:
                c.wait()

        out = call.run(body, held + 2**20, step)
        token = out["token"]
        if spread:
            columns = (out["share"], out["gain"])
        if mix:
            c = plan["mix"]
            kept[c] = out["kept"]
            peaks[c] = [out["peak"]] + [lax.ppermute(out["peak"], AXIS, p) for p in perms]
        if slim is not None:
            narrow[slim] = out["narrow"]
            pieces[slim] = [lax.ppermute(out["narrow"], AXIS, p) for p in perms]
        if "scales" in plan:
            scales = [out[f"scale{a}"].reshape(wd) for a, wd in enumerate(widths)]
        for a in touched:
            finals[a] = out[f"final{a}"]
    return (finals[0], finals[1], finals[2], *scales)


def solution(mesh):
    split = P(("job", AXIS), "cols")
    whole = P("job", "cols")
    vec = P(("job", "cols"))
    return jax.shard_map(
        make(mesh.shape[AXIS]),
        mesh=mesh,
        in_specs=(split,) * 6 + (P(("job", AXIS)),) * 2,
        out_specs=(whole, whole, whole, vec, vec, vec),
        check_vma=False,
    )
```
